32 devices in a mesh: pair: 2 (over x), tp: 4 (over z), side: 4 (over y, core).
Axes of the slice: x: 2, y: 2, z: 4, core: 2. Of those that a mesh axis runs over, the one named last changes fastest.
Arguments:
- x_prompt: bfloat16 [8, 512, 5120], P(('pair', 'side')), parts along dimension 0
- s_len: int32 [8], P(('pair', 'side')), parts along dimension 0
- y_tok: bfloat16 [8, 2, 5120], P(('pair', 'side')), parts along dimension 0
- k_cache: bfloat16 [8, 1, 2, 128, 128, 192], P(('pair', 'side'), None, None, None, 'tp'), parts along dimension 0
- v_cache: bfloat16 [8, 1, 2, 128, 128, 128], P(('pair', 'side'), None, None, None, 'tp'), parts along dimension 0
- c_len: int32 [8, 2], P(('pair', 'side')), parts along dimension 0
- attn_gain: bfloat16 [1, 5120], replicated
- w_q: bfloat16 [1, 5120, 128, 192], P(None, None, 'tp')
- w_dkv: bfloat16 [1, 5120, 576], replicated
- w_uk: bfloat16 [1, 512, 128, 128], P(None, None, 'tp')
- w_uv: bfloat16 [1, 512, 128, 128], P(None, None, 'tp')
- w_o: bfloat16 [1, 128, 128, 5120], P(None, 'tp')
- mlp_gain: bfloat16 [1, 5120], replicated
- w_gate: bfloat16 [1, 5120, 12288], P(None, None, 'tp')
- w_up: bfloat16 [1, 5120, 12288], P(None, None, 'tp')
- w_down: bfloat16 [1, 12288, 5120], P(None, 'tp')
Outputs:
- output 1: bfloat16 [8, 512, 5120], P(('pair', 'side')), parts along dimension 0
- output 2: bfloat16 [8, 2, 5120], P(('pair', 'side')), parts along dimension 0
- output 3: bfloat16 [8, 1, 512, 128, 192], P(('pair', 'side'), None, None, 'tp'), parts along dimension 0
- output 4: bfloat16 [8, 1, 512, 128, 128], P(('pair', 'side'), None, None, 'tp'), parts along dimension 0
- output 5: bfloat16 [8, 1, 2, 128, 128, 192], P(('pair', 'side'), None, None, None, 'tp'), parts along dimension 0
- output 6: bfloat16 [8, 1, 2, 128, 128, 128], P(('pair', 'side'), None, None, None, 'tp'), parts along dimension 0
There are 2 independent parts. The reference program is written for one: setup_inputs(seed, part) draws one part's arguments, and reference() takes and returns one part's arrays. A program takes and returns all parts, laid end to end along the dimension named above; an argument that names none is the same for every part.
All inputs are finite; a program needn't handle non-finite values.
Results may differ from the reference program's by a relative error of at most 0.0108281.
Values are sent between devices in bfloat16 or wider.
A program may use at most 1 GiB of HBM per device.

```python
import math
import jax
import jax.numpy as jnp
from jax import lax

GROUPS = 4
PROMPT = 512
BATCH = 2
CACHE = 128
LAYERS = 1
DMODEL = 5120
HEADS = 128
NOPE = 128
ROPE_DIM = 64
VDIM = 128
KV_RANK = 512
FFN = 12288
QK_DIM = NOPE + ROPE_DIM
SCALE_QK = QK_DIM ** -0.5
Q_SCALE = (math.log(PROMPT) / 2.0) ** 0.5
EPSILON = 1e-6
THETA = 10000.0


def normal_bf16(key_in, dim_list, scale_val):
    return (jax.random.normal(key_in, dim_list, jnp.float32) * scale_val).astype(jnp.bfloat16)


def setup_inputs(seed: int = 0, part: int = 0) -> dict:
    part_keys = jax.random.split(jax.random.fold_in(jax.random.key(seed), part), 6)
    shared_keys = jax.random.split(jax.random.key(seed + 1), 10)
    s_len = jax.random.randint(part_keys[1], (GROUPS,), PROMPT // 2, PROMPT + 1).at[0].set(PROMPT)
    c_len = jax.random.randint(part_keys[5], (GROUPS, BATCH), CACHE // 2, CACHE).at[:, 0].set(CACHE - 1)
    return {
        'x_prompt': normal_bf16(part_keys[0], (GROUPS, PROMPT, DMODEL), 1.0),
        's_len': s_len,
        'y_tok': normal_bf16(part_keys[2], (GROUPS, BATCH, DMODEL), 1.0),
        'k_cache': normal_bf16(part_keys[3], (GROUPS, LAYERS, BATCH, CACHE, HEADS, QK_DIM), 1.0),
        'v_cache': normal_bf16(part_keys[4], (GROUPS, LAYERS, BATCH, CACHE, HEADS, VDIM), 1.0),
        'c_len': c_len,
        'attn_gain': jax.random.uniform(shared_keys[0], (LAYERS, DMODEL), jnp.float32, 0.5, 1.5).astype(jnp.bfloat16),
        'w_q': normal_bf16(shared_keys[1], (LAYERS, DMODEL, HEADS, QK_DIM), Q_SCALE * DMODEL ** -0.5),
        'w_dkv': normal_bf16(shared_keys[2], (LAYERS, DMODEL, KV_RANK + ROPE_DIM), DMODEL ** -0.5),
        'w_uk': normal_bf16(shared_keys[3], (LAYERS, KV_RANK, HEADS, NOPE), KV_RANK ** -0.5),
        'w_uv': normal_bf16(shared_keys[4], (LAYERS, KV_RANK, HEADS, VDIM), KV_RANK ** -0.5),
        'w_o': normal_bf16(shared_keys[5], (LAYERS, HEADS, VDIM, DMODEL), 2.0 * (HEADS * VDIM) ** -0.5),
        'mlp_gain': jax.random.uniform(shared_keys[6], (LAYERS, DMODEL), jnp.float32, 0.5, 1.5).astype(jnp.bfloat16),
        'w_gate': normal_bf16(shared_keys[7], (LAYERS, DMODEL, FFN), DMODEL ** -0.5),
        'w_up': normal_bf16(shared_keys[8], (LAYERS, DMODEL, FFN), DMODEL ** -0.5),
        'w_down': normal_bf16(shared_keys[9], (LAYERS, FFN, DMODEL), FFN ** -0.5),
    }


def mixed_einsum(form, left, right):
    return jnp.einsum(form, left.astype(jnp.float32), right.astype(jnp.float32))


def rms_scaled(values, gain):
    hidden = values.astype(jnp.float32)
    inv_rms = lax.rsqrt(jnp.mean(hidden * hidden, axis=-1, keepdims=True) + EPSILON)
    return (hidden * inv_rms * gain.astype(jnp.float32)).astype(jnp.bfloat16)


def rms_plain(values):
    hidden = values.astype(jnp.float32)
    inv_rms = lax.rsqrt(jnp.mean(hidden * hidden, axis=-1, keepdims=True) + EPSILON)
    return (hidden * inv_rms).astype(jnp.bfloat16)


def apply_rope(values, positions):
    half_dim = values.shape[-1] // 2
    inv_freq = THETA ** (-jnp.arange(half_dim, dtype=jnp.float32) * 2.0 / values.shape[-1])
    angles = positions.astype(jnp.float32)[..., None] * inv_freq
    cos_part = jnp.cos(angles)
    sin_part = jnp.sin(angles)
    first_half = values[..., :half_dim].astype(jnp.float32)
    second_half = values[..., half_dim:].astype(jnp.float32)
    return jnp.concatenate([first_half * cos_part - second_half * sin_part, second_half * cos_part + first_half * sin_part], axis=-1).astype(jnp.bfloat16)


def mlp_block(normed, w_gate_l, w_up_l, w_down_l):
    gate_val = jnp.dot(normed, w_gate_l, preferred_element_type=jnp.float32)
    up_val = jnp.dot(normed, w_up_l, preferred_element_type=jnp.float32)
    act_val = (jax.nn.silu(gate_val) * up_val).astype(jnp.bfloat16)
    return jnp.dot(act_val, w_down_l, preferred_element_type=jnp.float32).astype(jnp.bfloat16)


def prefill_group(x_one, len_one, weights):
    positions = jnp.arange(PROMPT)
    allowed = (positions[None, :] <= positions[:, None]) & (positions[None, :] < len_one)

    def head_attention(head_item):
        q_head, k_head, v_head = head_item
        scores = jnp.dot(q_head, k_head.T, preferred_element_type=jnp.float32) * SCALE_QK
        probs_bf = jax.nn.softmax(jnp.where(allowed, scores, -1e30), axis=-1).astype(jnp.bfloat16)
        return jnp.dot(probs_bf, v_head, preferred_element_type=jnp.float32).astype(jnp.bfloat16)

    def layer_step(hidden, layer_w):
        gain_attn, w_q_l, w_dkv_l, w_uk_l, w_uv_l, w_o_l, gain_mlp, w_gate_l, w_up_l, w_down_l = layer_w
        normed = rms_scaled(hidden, gain_attn)
        query_all = mixed_einsum('sd,dhe->she', normed, w_q_l).astype(jnp.bfloat16)
        query_all = jnp.concatenate([query_all[:, :, :NOPE], apply_rope(query_all[:, :, NOPE:], positions[:, None])], axis=-1)
        latent_raw = jnp.dot(normed, w_dkv_l, preferred_element_type=jnp.float32).astype(jnp.bfloat16)
        latent = rms_plain(latent_raw[:, :KV_RANK])
        rope_key = apply_rope(latent_raw[:, KV_RANK:], positions)
        key_nope = mixed_einsum('sr,rhn->shn', latent, w_uk_l).astype(jnp.bfloat16)
        value_full = mixed_einsum('sr,rhv->shv', latent, w_uv_l).astype(jnp.bfloat16)
        key_full = jnp.concatenate([key_nope, jnp.broadcast_to(rope_key[:, None, :], (PROMPT, HEADS, ROPE_DIM))], axis=-1)
        attn_heads = lax.map(head_attention, (jnp.transpose(query_all, (1, 0, 2)), jnp.transpose(key_full, (1, 0, 2)), jnp.transpose(value_full, (1, 0, 2))))
        hidden = hidden + mixed_einsum('hsv,hvd->sd', attn_heads, w_o_l).astype(jnp.bfloat16)
        hidden = hidden + mlp_block(rms_scaled(hidden, gain_mlp), w_gate_l, w_up_l, w_down_l)
        return hidden, (key_full, value_full)

    hidden_out, cache_pair = lax.scan(layer_step, x_one, weights)
    return hidden_out, cache_pair[0], cache_pair[1]


def decode_group(y_one, k_one, v_one, len_vec, weights):
    slot_hit = (jnp.arange(CACHE)[None, :] == len_vec[:, None])[:, :, None, None]
    allowed = jnp.arange(CACHE)[None, None, :] <= len_vec[:, None, None]

    def layer_step(tok_state, layer_in):
        layer_w, key_old, value_old = layer_in
        gain_attn, w_q_l, w_dkv_l, w_uk_l, w_uv_l, w_o_l, gain_mlp, w_gate_l, w_up_l, w_down_l = layer_w
        normed = rms_scaled(tok_state, gain_attn)
        query_all = mixed_einsum('bd,dhe->bhe', normed, w_q_l).astype(jnp.bfloat16)
        query_all = jnp.concatenate([query_all[:, :, :NOPE], apply_rope(query_all[:, :, NOPE:], len_vec[:, None])], axis=-1)
        latent_raw = jnp.dot(normed, w_dkv_l, preferred_element_type=jnp.float32).astype(jnp.bfloat16)
        latent = rms_plain(latent_raw[:, :KV_RANK])
        rope_key = apply_rope(latent_raw[:, KV_RANK:], len_vec)
        key_nope = mixed_einsum('br,rhn->bhn', latent, w_uk_l).astype(jnp.bfloat16)
        value_new = mixed_einsum('br,rhv->bhv', latent, w_uv_l).astype(jnp.bfloat16)
        key_new = jnp.concatenate([key_nope, jnp.broadcast_to(rope_key[:, None, :], (BATCH, HEADS, ROPE_DIM))], axis=-1)
        key_layer = jnp.where(slot_hit, key_new[:, None], key_old)
        value_layer = jnp.where(slot_hit, value_new[:, None], value_old)
        scores = mixed_einsum('bhe,bthe->bht', query_all, key_layer) * SCALE_QK
        probs_bf = jax.nn.softmax(jnp.where(allowed, scores, -1e30), axis=-1).astype(jnp.bfloat16)
        attn_val = mixed_einsum('bht,bthv->bhv', probs_bf, value_layer).astype(jnp.bfloat16)
        tok_state = tok_state + mixed_einsum('bhv,hvd->bd', attn_val, w_o_l).astype(jnp.bfloat16)
        tok_state = tok_state + mlp_block(rms_scaled(tok_state, gain_mlp), w_gate_l, w_up_l, w_down_l)
        return tok_state, (key_layer, value_layer)

    tok_out, cache_pair = lax.scan(layer_step, y_one, (weights, k_one, v_one))
    return tok_out, cache_pair[0], cache_pair[1]


def reference(x_prompt, s_len, y_tok, k_cache, v_cache, c_len, attn_gain, w_q, w_dkv, w_uk, w_uv, w_o, mlp_gain, w_gate, w_up, w_down):
    weights = (attn_gain, w_q, w_dkv, w_uk, w_uv, w_o, mlp_gain, w_gate, w_up, w_down)

    def prefill_one(group_item):
        return prefill_group(group_item[0], group_item[1], weights)

    def decode_one(group_item):
        return decode_group(group_item[0], group_item[1], group_item[2], group_item[3], weights)

    hidden_out, key_all, value_all = lax.map(prefill_one, (x_prompt, s_len))
    tok_out, key_next, value_next = lax.map(decode_one, (y_tok, k_cache, v_cache, c_len))
    return (hidden_out, tok_out, jnp.roll(key_all, 1, axis=0), jnp.roll(value_all, 1, axis=0), key_next, value_next)
```

```python
import functools

import jax
import jax.numpy as jnp
from jax import lax
from jax.experimental import pallas as pl
from jax.experimental.pallas import tpu as pltpu
from jax.sharding import PartitionSpec as P

EPSILON = 1e-6
THETA = 10000.0

SUB = 128
CHUNK = 2 * SUB
LAG = 2
RING_OWN = 16
RING_LAND = 32
RING_SEND = 16
DEC = 8
MESH = pl.DeviceIdType.MESH


def rms_scaled(values, gain):
    hidden = values.astype(jnp.float32)
    inv_rms = lax.rsqrt(jnp.mean(hidden * hidden, axis=-1, keepdims=True) + EPSILON)
    return (hidden * inv_rms * gain.astype(jnp.float32)).astype(jnp.bfloat16)


def rms_plain(values):
    hidden = values.astype(jnp.float32)
    inv_rms = lax.rsqrt(jnp.mean(hidden * hidden, axis=-1, keepdims=True) + EPSILON)
    return (hidden * inv_rms).astype(jnp.bfloat16)


def apply_rope(values, positions):
    half_dim = values.shape[-1] // 2
    inv_freq = THETA ** (-jnp.arange(half_dim, dtype=jnp.float32) * 2.0 / values.shape[-1])
    angles = positions.astype(jnp.float32)[..., None] * inv_freq
    cos_part = jnp.cos(angles)
    sin_part = jnp.sin(angles)
    first_half = values[..., :half_dim].astype(jnp.float32)
    second_half = values[..., half_dim:].astype(jnp.float32)
    return jnp.concatenate([first_half * cos_part - second_half * sin_part, second_half * cos_part + first_half * sin_part], axis=-1).astype(jnp.bfloat16)


def make_query(normed, w_q_layer, positions, nope_dim):
    query_all = jnp.einsum('sd,dhe->she', normed, w_q_layer, preferred_element_type=jnp.float32).astype(jnp.bfloat16)
    return jnp.concatenate([query_all[..., :nope_dim], apply_rope(query_all[..., nope_dim:], positions[:, None])], axis=-1)


def make_latent(normed, w_dkv_layer, positions, rank_dim):
    latent_raw = jnp.dot(normed, w_dkv_layer, preferred_element_type=jnp.float32).astype(jnp.bfloat16)
    return jnp.concatenate([rms_plain(latent_raw[:, :rank_dim]), apply_rope(latent_raw[:, rank_dim:], positions)], axis=-1)


def expand_latent(latent_pack, w_uk_layer, w_uv_layer):
    rank_dim = w_uk_layer.shape[0]
    latent = latent_pack[:, :rank_dim]
    rope_key = latent_pack[:, rank_dim:]
    key_nope = jnp.einsum('sr,rhn->shn', latent, w_uk_layer, preferred_element_type=jnp.float32).astype(jnp.bfloat16)
    value_full = jnp.einsum('sr,rhv->shv', latent, w_uv_layer, preferred_element_type=jnp.float32).astype(jnp.bfloat16)
    rope_heads = jnp.broadcast_to(rope_key[:, None, :], (key_nope.shape[0], key_nope.shape[1], rope_key.shape[1]))
    return jnp.concatenate([key_nope, rope_heads], axis=-1), value_full


def masked_softmax(scores, allowed):
    return jax.nn.softmax(jnp.where(allowed, scores, -1e30), axis=-1).astype(jnp.bfloat16)


def prompt_attention(query_all, key_full, value_full, valid_len):
    seq_len = query_all.shape[0]
    scores = jnp.einsum('qhe,khe->hqk', query_all, key_full, preferred_element_type=jnp.float32) * query_all.shape[-1] ** -0.5
    row_pos = jnp.arange(seq_len)[:, None]
    col_pos = jnp.arange(seq_len)[None, :]
    allowed = (col_pos <= row_pos) & (col_pos < valid_len)
    probs_bf = masked_softmax(scores, allowed[None])
    return jnp.einsum('hqk,khv->qhv', probs_bf, value_full, preferred_element_type=jnp.float32).astype(jnp.bfloat16)


def cache_attention(query_all, key_layer, value_layer, cur_len):
    scores = jnp.einsum('bhe,bthe->bht', query_all, key_layer, preferred_element_type=jnp.float32) * query_all.shape[-1] ** -0.5
    allowed = jnp.arange(key_layer.shape[1])[None, None, :] <= cur_len[:, None, None]
    probs_bf = masked_softmax(scores, allowed)
    return jnp.einsum('bht,bthv->bhv', probs_bf, value_layer, preferred_element_type=jnp.float32).astype(jnp.bfloat16)


def block_kernel(n_tp, ap_ref, ad_ref, gain_ref, x_hbm, ys_hbm, wo_hbm, wg_hbm, wu_hbm, wd_hbm, out_hbm, outd_hbm,
                 hb, own, land, dec, wa, wb, b_buf, act, stat,
                 wa_sem, wb_sem, x_sem, out_sem, outd_sem, rs_send, rs_recv, ag_send, ag_recv):
    last = n_tp - 1
    hv = wo_hbm.shape[0]
    dm = wo_hbm.shape[1]
    ffn = wg_hbm.shape[1]
    half = dm // 2
    nt = half // SUB
    nf = ffn // SUB
    units = 2 * (2 * nt + 1)
    total = 2 * units
    z = lax.axis_index('tp')

    barrier = pltpu.get_barrier_semaphore()

    @pl.when(z > 0)
    def _():
        pl.semaphore_signal(barrier, inc=1, device_id={'tp': z - 1}, device_id_type=MESH)

    @pl.when(z < last)
    def _():
        pl.semaphore_signal(barrier, inc=1, device_id={'tp': z + 1}, device_id_type=MESH)

    pos = (z, last - z)
    nxt = (z + 1, z - 1)
    prv = (z - 1, z + 1)

    def wo_copies(q):
        slot = q % 3
        j = q % nt
        return [pltpu.make_async_copy(wo_hbm.at[:, pl.ds(pl.multiple_of(d * half + j * SUB, SUB), SUB)],
                                      wa.at[slot, pl.ds(0, hv), pl.ds(d * SUB, SUB)], wa_sem.at[slot]) for d in (0, 1)]

    def wd_copies(q):
        slot = q % 3
        j = q % nt
        return [pltpu.make_async_copy(wd_hbm.at[:, pl.ds(pl.multiple_of(d * half + j * SUB, SUB), SUB)],
                                      wa.at[slot, pl.ds(0, ffn), pl.ds(d * SUB, SUB)], wa_sem.at[slot]) for d in (0, 1)]

    def start_a(q):
        @pl.when(q < 2 * nt)
        def _():
            for copy in wo_copies(q):
                copy.start()

        @pl.when((q >= 2 * nt) & (q < 4 * nt))
        def _():
            for copy in wd_copies(q):
                copy.start()

    def start_b(q):
        @pl.when(q < 2 * nf)
        def _():
            slot = q % 3
            j = q % nf
            cols = pl.ds(pl.multiple_of(j * SUB, SUB), SUB)
            pltpu.make_async_copy(wg_hbm.at[:, cols], wb.at[slot, :, pl.ds(0, SUB)], wb_sem.at[slot]).start()
            pltpu.make_async_copy(wu_hbm.at[:, cols], wb.at[slot, :, pl.ds(SUB, SUB)], wb_sem.at[slot]).start()

    start_a(0)
    start_a(1)
    start_b(0)
    start_b(1)

    def x_copy(d, w):
        i = w // 2
        rows = pl.ds(pl.multiple_of((i // nt) * CHUNK + (w % 2) * SUB, SUB), SUB)
        cols = pl.ds(pl.multiple_of(d * half + (i % nt) * SUB, SUB), SUB)
        return rows, cols

    for d in (0, 1):
        @pl.when(pos[d] == last)
        def _():
            @pl.loop(0, 4 * nt)
            def _(w):
                rows, cols = x_copy(d, w)
                pltpu.make_async_copy(x_hbm.at[rows, cols], hb.at[d, w], x_sem).start()
            for s in (0, 1):
                pltpu.make_async_copy(ys_hbm.at[d, s], hb.at[d, 4 * nt + s], x_sem).start()

    dec[...] = jnp.zeros_like(dec)

    pl.semaphore_wait(barrier, jnp.where(z > 0, 1, 0) + jnp.where(z < last, 1, 0))

    for d in (0, 1):
        @pl.when(pos[d] == last)
        def _():
            pltpu.make_async_copy(hb.at[d, pl.ds(0, units)], hb.at[d, pl.ds(0, units)], x_sem).wait()

    def rs_copy(d, u):
        return pltpu.make_async_remote_copy(
            src_ref=own.at[d, u % RING_OWN], dst_ref=land.at[d, u % RING_LAND],
            send_sem=rs_send.at[d, u % RING_OWN], recv_sem=rs_recv.at[d, u % RING_LAND],
            device_id={'tp': nxt[d]}, device_id_type=MESH)

    def ag_copy(d, u):
        return pltpu.make_async_remote_copy(
            src_ref=hb.at[d, u], dst_ref=hb.at[d, u],
            send_sem=ag_send.at[d, u % RING_SEND], recv_sem=ag_recv.at[d, u % RING_LAND],
            device_id={'tp': prv[d]}, device_id_type=MESH)

    def give_back(d, u):
        @pl.when(u >= RING_SEND)
        def _():
            ag_copy(d, u).wait_send()
        ag_copy(d, u).start()

    def write_out(d, u):
        w = u - units

        @pl.when((w >= 0) & (w < 4 * nt))
        def _():
            rows, cols = x_copy(d, w)
            pltpu.make_async_copy(hb.at[d, u], out_hbm.at[rows, cols], out_sem).start()

        @pl.when(w >= 4 * nt)
        def _():
            pltpu.make_async_copy(hb.at[d, u], outd_hbm.at[d, w - 4 * nt], outd_sem).start()

    def tick(t):
        for d in (0, 1):
            p = pos[d]
            u = t - LAG * p

            @pl.when((u >= 0) & (u < total))
            def _():
                @pl.when(p == 0)
                def _():
                    rs_copy(d, u).start()

                @pl.when((p > 0) & (p < last))
                def _():
                    rs_copy(d, u).wait_recv()
                    own[d, u % RING_OWN] = own[d, u % RING_OWN] + land[d, u % RING_LAND]
                    rs_copy(d, u).start()

                @pl.when(p == last)
                def _():
                    rs_copy(d, u).wait_recv()
                    summed = (own[d, u % RING_OWN] + land[d, u % RING_LAND]).astype(jnp.bfloat16)
                    hb[d, u] = (hb[d, u % units].astype(jnp.float32) + summed.astype(jnp.float32)).astype(jnp.bfloat16)
                    give_back(d, u)
                    write_out(d, u)

        for d in (0, 1):
            p = pos[d]
            v = t - LAG * (2 * last - p)

            @pl.when((p < last) & (v >= 0) & (v < total))
            def _():
                ag_copy(d, v).wait_recv()

                @pl.when(p > 0)
                def _():
                    give_back(d, v)
                write_out(d, v)

    def free_own(i):
        for d in (0, 1):
            for s in (0, 1):
                u = 2 * i + s

                @pl.when((u >= RING_OWN) & (pos[d] < last))
                def _():
                    rs_copy(d, u).wait_send()

    def store_own(i, q, res, has_dec):
        free_own(i)
        for d in (0, 1):
            for s in (0, 1):
                own[d, (2 * i + s) % RING_OWN] = res[s * SUB:(s + 1) * SUB, d * SUB:(d + 1) * SUB]
            if has_dec:
                j = q % nt
                dec[d, pl.ds(pl.multiple_of(j * DEC, DEC), DEC), :] = res[CHUNK:CHUNK + DEC, d * SUB:(d + 1) * SUB]

    def wo_step(i, q, chunk):
        start_a(q + 2)
        slot = q % 3
        pltpu.make_async_copy(wa.at[slot, pl.ds(0, hv)], wa.at[slot, pl.ds(0, hv)], wa_sem.at[slot]).wait()
        if chunk == 0:
            lhs = ap_ref[0:CHUNK, :]
        else:
            lhs = jnp.concatenate([ap_ref[CHUNK:2 * CHUNK, :], ad_ref[...]], axis=0)
        res = jnp.dot(lhs, wa[slot, 0:hv, :], preferred_element_type=jnp.float32)
        store_own(i, q, res, chunk == 1)

    def down_step(i, q, chunk):
        start_a(q + 2)
        slot = q % 3
        pltpu.make_async_copy(wa.at[slot, pl.ds(0, ffn)], wa.at[slot, pl.ds(0, ffn)], wa_sem.at[slot]).wait()
        lhs = act[chunk, 0:CHUNK, :] if chunk == 0 else act[chunk]
        res = jnp.dot(lhs, wa[slot, 0:ffn, :], preferred_element_type=jnp.float32)
        store_own(i, q, res, chunk == 1)

    def gu_step(q, chunk):
        start_b(q + 2)
        slot = q % 3
        pltpu.make_async_copy(wb.at[slot], wb.at[slot], wb_sem.at[slot]).wait()
        rows = CHUNK if chunk == 0 else CHUNK + 2 * DEC
        res = jnp.dot(b_buf[0:rows, :], wb[slot], preferred_element_type=jnp.float32)
        j = q % nf
        value = (jax.nn.silu(res[:, :SUB]) * res[:, SUB:]).astype(jnp.bfloat16)
        act[chunk, 0:rows, pl.ds(pl.multiple_of(j * SUB, SUB), SUB)] = value

    def norm_chunk(chunk):
        for s in (0, 1):
            stat[...] = jnp.zeros_like(stat)

            @pl.loop(0, nt)
            def _(j):
                for d in (0, 1):
                    hid = hb[d, 2 * (chunk * nt + j) + s].astype(jnp.float32)
                    stat[...] = stat[...] + hid * hid
            inv = lax.rsqrt(jnp.sum(stat[...], axis=-1, keepdims=True) * (1.0 / dm) + EPSILON)
            stat[...] = jnp.broadcast_to(inv, stat.shape)

            @pl.loop(0, nt)
            def _(j):
                for d in (0, 1):
                    cols = pl.ds(pl.multiple_of(d * half + j * SUB, SUB), SUB)
                    hid = hb[d, 2 * (chunk * nt + j) + s].astype(jnp.float32)
                    b_buf[s * SUB:(s + 1) * SUB, cols] = (hid * stat[...] * gain_ref[:, cols].astype(jnp.float32)).astype(jnp.bfloat16)

    def norm_dec():
        per = SUB // DEC
        tiles = []
        for d in (0, 1):
            both = [hb[d, 4 * nt + s].astype(jnp.float32) for s in (0, 1)]
            for j in range(nt):
                r = (j % per) * DEC
                tiles.append(both[j // per][r:r + DEC, :])
        square = tiles[0] * tiles[0]
        for tile in tiles[1:]:
            square = square + tile * tile
        inv = lax.rsqrt(jnp.sum(square, axis=-1, keepdims=True) * (1.0 / dm) + EPSILON)
        pad = jnp.zeros((DEC, SUB), jnp.float32)
        for k, tile in enumerate(tiles):
            value = tile * inv * gain_ref[:, k * SUB:(k + 1) * SUB].astype(jnp.float32)
            b_buf[CHUNK:CHUNK + 2 * DEC, k * SUB:(k + 1) * SUB] = jnp.concatenate([value, pad], axis=0).astype(jnp.bfloat16)

    def dec_unit(i):
        free_own(i)
        for d in (0, 1):
            for s in (0, 1):
                own[d, (2 * i + s) % RING_OWN] = dec[d, s * SUB:(s + 1) * SUB, :]

    wait_units = (2 * nt - 1 + 2 * last * LAG) // 2 + 1
    wait_all = (4 * nt + 1 + 2 * last * LAG) // 2 + 1

    @pl.loop(0, nt)
    def _(i):
        wo_step(i, i, 0)
        tick(2 * i)
        tick(2 * i + 1)

    @pl.loop(nt, wait_units)
    def _(i):
        wo_step(i, i, 1)
        tick(2 * i)
        tick(2 * i + 1)

    norm_chunk(0)
    mid0 = wait_units + nf // 2

    @pl.loop(wait_units, mid0)
    def _(i):
        wo_step(i, i, 1)
        tick(2 * i)
        gu_step(2 * (i - wait_units), 0)
        tick(2 * i + 1)
        gu_step(2 * (i - wait_units) + 1, 0)

    @pl.loop(mid0, 2 * nt)
    def _(i):
        wo_step(i, i, 1)
        tick(2 * i)
        tick(2 * i + 1)

    dec_unit(2 * nt)
    tick(4 * nt)
    tick(4 * nt + 1)

    first = 2 * nt + 1

    @pl.loop(first, wait_all)
    def _(i):
        down_step(i, i - 1, 0)
        tick(2 * i)
        tick(2 * i + 1)

    norm_chunk(1)
    norm_dec()
    mid1 = wait_all + nf // 2

    @pl.loop(wait_all, mid1)
    def _(i):
        down_step(i, i - 1, 0)
        tick(2 * i)
        gu_step(nf + 2 * (i - wait_all), 1)
        tick(2 * i + 1)
        gu_step(nf + 2 * (i - wait_all) + 1, 1)

    @pl.loop(mid1, first + nt)
    def _(i):
        down_step(i, i - 1, 0)
        tick(2 * i)
        tick(2 * i + 1)

    @pl.loop(first + nt, first + 2 * nt)
    def _(i):
        down_step(i, i - 1, 1)
        tick(2 * i)
        tick(2 * i + 1)

    dec_unit(first + 2 * nt)

    @pl.loop(total - 2, total + 2 * last * LAG)
    def _(t):
        tick(t)

    for d in (0, 1):
        @pl.when(pos[d] < last)
        def _():
            @pl.loop(total - RING_OWN, total)
            def _(u):
                rs_copy(d, u).wait_send()

        @pl.when(pos[d] > 0)
        def _():
            @pl.loop(total - RING_SEND, total)
            def _(u):
                ag_copy(d, u).wait_send()

    pltpu.make_async_copy(hb.at[:, pl.ds(units, 4 * nt)], hb.at[:, pl.ds(units, 4 * nt)], out_sem).wait()
    pltpu.make_async_copy(hb.at[:, pl.ds(0, 2)], hb.at[:, pl.ds(0, 2)], outd_sem).wait()


def finish_block(n_tp, attn_prompt, attn_tok, mlp_gain, x_rows, y_stack, w_o, w_gate, w_up, w_down):
    dm = x_rows.shape[1]
    hv = w_o.shape[0]
    ffn = w_gate.shape[1]
    nt = dm // 2 // SUB
    units = 2 * (2 * nt + 1)
    bf, f32 = jnp.bfloat16, jnp.float32
    vmem = pl.BlockSpec(memory_space=pltpu.VMEM)
    hbm = pl.BlockSpec(memory_space=pl.ANY)
    sem = pltpu.SemaphoreType.DMA
    return pl.pallas_call(
        functools.partial(block_kernel, n_tp),
        out_shape=(jax.ShapeDtypeStruct(x_rows.shape, bf), jax.ShapeDtypeStruct((2, 2, SUB, SUB), bf)),
        in_specs=[vmem, vmem, vmem, hbm, hbm, hbm, hbm, hbm, hbm],
        out_specs=(hbm, hbm),
        scratch_shapes=[
            pltpu.VMEM((2, 2 * units, SUB, SUB), bf),
            pltpu.VMEM((2, RING_OWN, SUB, SUB), f32),
            pltpu.VMEM((2, RING_LAND, SUB, SUB), f32),
            pltpu.VMEM((2, CHUNK, SUB), f32),
            pltpu.VMEM((3, max(hv, ffn), 2 * SUB), bf),
            pltpu.VMEM((3, dm, 2 * SUB), bf),
            pltpu.VMEM((CHUNK + 2 * DEC, dm), bf),
            pltpu.VMEM((2, CHUNK + 2 * DEC, ffn), bf),
            pltpu.VMEM((SUB, SUB), f32),
            sem((3,)), sem((3,)), sem, sem, sem,
            sem((2, RING_OWN)), sem((2, RING_LAND)), sem((2, RING_SEND)), sem((2, RING_LAND)),
        ],
        compiler_params=pltpu.CompilerParams(collective_id=0, has_side_effects=True, vmem_limit_bytes=64000 * 1024),
    )(attn_prompt, attn_tok, mlp_gain, x_rows, y_stack, w_o, w_gate, w_up, w_down)


def stack_tokens(rows):
    nb, dm = rows.shape
    nt = dm // 2 // SUB
    tiles = jnp.transpose(rows.reshape(nb, 2, nt, SUB), (1, 2, 0, 3))
    tiles = jnp.pad(tiles, ((0, 0), (0, CHUNK // DEC - nt), (0, DEC - nb), (0, 0)))
    return tiles.reshape(2, 2, SUB, SUB)


def unstack_tokens(stack, nb, dm):
    nt = dm // 2 // SUB
    tiles = stack.reshape(2, CHUNK // DEC, DEC, SUB)[:, :nt, :nb]
    return jnp.transpose(tiles, (2, 0, 1, 3)).reshape(nb, dm)


def solution(mesh):
    groups = mesh.shape['side']
    n_tp = mesh.shape['tp']
    shift_pairs = [(source_idx, (source_idx + 1) % groups) for source_idx in range(groups)]
    group_axes = ('pair', 'side')
    head_spec = P(None, None, 'tp', None)
    cache_spec = P(group_axes, None, None, None, 'tp', None)
    prompt_spec = P(group_axes, None, None, 'tp', None)
    row_spec = P(group_axes, None, None)
    spec_in = (row_spec, P(group_axes), row_spec, cache_spec, cache_spec, P(group_axes, None), P(), head_spec, P(), head_spec, head_spec, P(None, 'tp', None, None), P(), P(None, None, 'tp'), P(None, None, 'tp'), P(None, 'tp', None))
    spec_out = (row_spec, row_spec, prompt_spec, prompt_spec, cache_spec, cache_spec)

    def device_step(x_prompt, s_len, y_tok, k_cache, v_cache, c_len, attn_gain, w_q, w_dkv, w_uk, w_uv, w_o, mlp_gain, w_gate, w_up, w_down):
        hidden = x_prompt[0]
        tok_state = y_tok[0]
        seq, dm = hidden.shape
        nb = tok_state.shape[0]
        cur_len = c_len[0]
        wq, wdkv, wuk, wuv = w_q[0], w_dkv[0], w_uk[0], w_uv[0]
        nope, rank = wuk.shape[-1], wuk.shape[0]
        key_old, value_old = k_cache[0, 0], v_cache[0, 0]

        rows = jnp.concatenate([hidden, tok_state], axis=0)
        positions = jnp.concatenate([jnp.arange(seq, dtype=jnp.int32), cur_len.astype(jnp.int32)])
        normed = rms_scaled(rows, attn_gain[0])
        latent_pack = make_latent(normed, wdkv, positions, rank)
        received = lax.ppermute(latent_pack[:seq], 'side', shift_pairs)
        query_all = make_query(normed, wq, positions, nope)
        key_all, value_all = expand_latent(latent_pack, wuk, wuv)
        attn_prompt = prompt_attention(query_all[:seq], key_all[:seq], value_all[:seq], s_len[0])

        slot_hit = (jnp.arange(key_old.shape[1])[None, :] == cur_len[:, None])[:, :, None, None]
        key_next = jnp.where(slot_hit, key_all[seq:, None], key_old)
        value_next = jnp.where(slot_hit, value_all[seq:, None], value_old)
        attn_tok = cache_attention(query_all[seq:], key_next, value_next, cur_len)

        hv = w_o.shape[1] * w_o.shape[2]
        attn_tok = jnp.pad(attn_tok.reshape(nb, hv), ((0, 2 * DEC - nb), (0, 0)))
        h_out, tok_out = finish_block(
            n_tp, attn_prompt.reshape(seq, hv), attn_tok, mlp_gain, hidden, stack_tokens(tok_state),
            w_o[0].reshape(hv, dm), w_gate[0], w_up[0], w_down[0])
        key_in, value_in = expand_latent(received, wuk, wuv)
        return (h_out[None], unstack_tokens(tok_out, nb, dm)[None], key_in[None, None], value_in[None, None], key_next[None, None], value_next[None, None])

    return jax.shard_map(device_step, mesh=mesh, in_specs=spec_in, out_specs=spec_out, check_vma=False)
```

```python
import functools

import jax
import jax.numpy as jnp
from jax import lax
from jax.experimental import pallas as pl
from jax.experimental.pallas import tpu as pltpu
from jax.sharding import PartitionSpec as P

EPSILON = 1e-6
THETA = 10000.0

SUB = 128
CHUNK = 2 * SUB
LAG = 2
RING_OWN = 16
RING_LAND = 32
RING_SEND = 16
RING_HEAD = 3
DEC = 8
MESH = pl.DeviceIdType.MESH


def rms_scaled(values, gain):
    hidden = values.astype(jnp.float32)
    inv_rms = lax.rsqrt(jnp.mean(hidden * hidden, axis=-1, keepdims=True) + EPSILON)
    return (hidden * inv_rms * gain.astype(jnp.float32)).astype(jnp.bfloat16)


def rms_plain(values):
    hidden = values.astype(jnp.float32)
    inv_rms = lax.rsqrt(jnp.mean(hidden * hidden, axis=-1, keepdims=True) + EPSILON)
    return (hidden * inv_rms).astype(jnp.bfloat16)


def apply_rope(values, positions):
    half_dim = values.shape[-1] // 2
    inv_freq = THETA ** (-jnp.arange(half_dim, dtype=jnp.float32) * 2.0 / values.shape[-1])
    angles = positions.astype(jnp.float32)[..., None] * inv_freq
    cos_part = jnp.cos(angles)
    sin_part = jnp.sin(angles)
    first_half = values[..., :half_dim].astype(jnp.float32)
    second_half = values[..., half_dim:].astype(jnp.float32)
    return jnp.concatenate([first_half * cos_part - second_half * sin_part, second_half * cos_part + first_half * sin_part], axis=-1).astype(jnp.bfloat16)


def make_latent(normed, w_dkv_layer, positions, rank_dim):
    latent_raw = jnp.dot(normed, w_dkv_layer, preferred_element_type=jnp.float32).astype(jnp.bfloat16)
    return jnp.concatenate([rms_plain(latent_raw[:, :rank_dim]), apply_rope(latent_raw[:, rank_dim:], positions)], axis=-1)


def block_kernel(n_tp, n_heads, scale, len_ref, clen_ref, kr_ref, cos_ref, sin_ref, rot_ref, gain_ref, a_ref,
                 wq_hbm, kn_hbm, v_hbm, kt_hbm, vt_hbm,
                 x_hbm, ys_hbm, wo_hbm, wg_hbm, wu_hbm, wd_hbm, out_hbm, outd_hbm,
                 hb, own, land, dec, wa, wb, b_buf, act, stat, attn, mask, wq_buf, kn_buf, v_buf, kt_buf, vt_buf,
                 wa_sem, wb_sem, x_sem, out_sem, outd_sem, rs_send, rs_recv, ag_send, ag_recv, att_sem):
    last = n_tp - 1
    hv = wo_hbm.shape[0]
    dm = wo_hbm.shape[1]
    ffn = wg_hbm.shape[1]
    half = dm // 2
    nt = half // SUB
    nf = ffn // SUB
    units = 2 * (2 * nt + 1)
    total = 2 * units
    z = lax.axis_index('tp')

    barrier = pltpu.get_barrier_semaphore()

    @pl.when(z > 0)
    def _():
        pl.semaphore_signal(barrier, inc=1, device_id={'tp': z - 1}, device_id_type=MESH)

    @pl.when(z < last)
    def _():
        pl.semaphore_signal(barrier, inc=1, device_id={'tp': z + 1}, device_id_type=MESH)

    pos = (z, last - z)
    nxt = (z + 1, z - 1)
    prv = (z - 1, z + 1)

    def wo_copies(q):
        slot = q % 3
        j = q % nt
        return [pltpu.make_async_copy(wo_hbm.at[:, pl.ds(pl.multiple_of(d * half + j * SUB, SUB), SUB)],
                                      wa.at[slot, pl.ds(0, hv), pl.ds(d * SUB, SUB)], wa_sem.at[slot]) for d in (0, 1)]

    def wd_copies(q):
        slot = q % 3
        j = q % nt
        return [pltpu.make_async_copy(wd_hbm.at[:, pl.ds(pl.multiple_of(d * half + j * SUB, SUB), SUB)],
                                      wa.at[slot, pl.ds(0, ffn), pl.ds(d * SUB, SUB)], wa_sem.at[slot]) for d in (0, 1)]

    def start_a(q):
        @pl.when(q < 2 * nt)
        def _():
            for copy in wo_copies(q):
                copy.start()

        @pl.when((q >= 2 * nt) & (q < 4 * nt))
        def _():
            for copy in wd_copies(q):
                copy.start()

    def start_b(q):
        @pl.when(q < 2 * nf)
        def _():
            slot = q % 3
            j = q % nf
            cols = pl.ds(pl.multiple_of(j * SUB, SUB), SUB)
            pltpu.make_async_copy(wg_hbm.at[:, cols], wb.at[slot, :, pl.ds(0, SUB)], wb_sem.at[slot]).start()
            pltpu.make_async_copy(wu_hbm.at[:, cols], wb.at[slot, :, pl.ds(SUB, SUB)], wb_sem.at[slot]).start()

    nope = kn_hbm.shape[-1]
    nb = kt_hbm.shape[0]
    tok_rows = slice(2 * CHUNK, 2 * CHUNK + 2 * DEC)

    def att_copies(g, chunk):
        slot = g % RING_HEAD
        keys = pl.ds(0, CHUNK * (chunk + 1))
        copies = [pltpu.make_async_copy(wq_hbm.at[g], wq_buf.at[slot], att_sem.at[0, slot]),
                  pltpu.make_async_copy(kn_hbm.at[g, keys], kn_buf.at[slot, keys], att_sem.at[1, slot]),
                  pltpu.make_async_copy(v_hbm.at[g, keys], v_buf.at[slot, keys], att_sem.at[2, slot])]
        if chunk == 0:
            for n in range(nb):
                copies.append(pltpu.make_async_copy(kt_hbm.at[n, g], kt_buf.at[slot, n], att_sem.at[3 + n, slot]))
                copies.append(pltpu.make_async_copy(vt_hbm.at[n, g], vt_buf.at[slot, n], att_sem.at[3 + nb + n, slot]))
        return copies

    def start_att(g, chunk):
        for copy in att_copies(g, chunk):
            copy.start()

    def take_rows(ref, chunk):
        if chunk == 0:
            return jnp.concatenate([ref[0:CHUNK, :], ref[tok_rows, :]], axis=0)
        return ref[CHUNK:2 * CHUNK, :]

    def softmax(scores):
        expd = jnp.exp(scores - jnp.max(scores, axis=-1, keepdims=True))
        return (expd * (1.0 / jnp.sum(expd, axis=-1, keepdims=True))).astype(jnp.bfloat16)

    def att_step(g, chunk):
        @pl.when(g + RING_HEAD - 1 < n_heads)
        def _():
            start_att(g + RING_HEAD - 1, chunk)
        for copy in att_copies(g, chunk):
            copy.wait()
        slot = g % RING_HEAD
        keys = CHUNK * (chunk + 1)
        rows = slice(chunk * CHUNK, (chunk + 1) * CHUNK)
        cols = pl.ds(pl.multiple_of(g * SUB, SUB), SUB)
        contract = (((1,), (1,)), ((), ()))
        f32, bf = jnp.float32, jnp.bfloat16
        query = lax.dot_general(take_rows(a_ref, chunk), wq_buf[slot], contract, preferred_element_type=f32).astype(bf)
        flat, raw = query[:, :nope], query[:, nope:]
        turned = jnp.dot(raw, rot_ref[...], preferred_element_type=f32)
        rope = (raw.astype(f32) * take_rows(cos_ref, chunk) + turned * take_rows(sin_ref, chunk)).astype(bf)
        scores = lax.dot_general(flat[:CHUNK], kn_buf[slot, 0:keys, :], contract, preferred_element_type=f32)
        scores = scores + lax.dot_general(rope[:CHUNK], kr_ref[0:keys, :], contract, preferred_element_type=f32)
        probs = softmax(jnp.where(mask[rows, 0:keys] > 0, scores * scale, -1e30))
        attn[rows, cols] = jnp.dot(probs, v_buf[slot, 0:keys, :], preferred_element_type=f32).astype(bf)
        if chunk == 0:
            total_tok = jnp.zeros((2 * DEC, SUB), f32)
            for n in range(nb):
                kt = kt_buf[slot, n]
                scores = jnp.dot(flat[CHUNK:], kt[:nope], preferred_element_type=f32)
                scores = (scores + jnp.dot(rope[CHUNK:], kt[nope:], preferred_element_type=f32)) * scale
                slots = lax.broadcasted_iota(jnp.int32, scores.shape, 1)
                probs = softmax(jnp.where(slots <= clen_ref[n:n + 1, :], scores, -1e30))
                value = jnp.dot(probs, vt_buf[slot, n], preferred_element_type=f32)
                row = lax.broadcasted_iota(jnp.int32, value.shape, 0)
                total_tok = jnp.where(row == n, value, total_tok)
            attn[tok_rows, cols] = total_tok.astype(bf)

    for g in range(RING_HEAD - 1):
        start_att(g, 0)
    start_a(0)
    start_a(1)
    start_b(0)
    start_b(1)

    def x_copy(d, w):
        i = w // 2
        rows = pl.ds(pl.multiple_of((i // nt) * CHUNK + (w % 2) * SUB, SUB), SUB)
        cols = pl.ds(pl.multiple_of(d * half + (i % nt) * SUB, SUB), SUB)
        return rows, cols

    for d in (0, 1):
        @pl.when(pos[d] == last)
        def _():
            @pl.loop(0, 4 * nt)
            def _(w):
                rows, cols = x_copy(d, w)
                pltpu.make_async_copy(x_hbm.at[rows, cols], hb.at[d, w], x_sem).start()
            for s in (0, 1):
                pltpu.make_async_copy(ys_hbm.at[d, s], hb.at[d, 4 * nt + s], x_sem).start()

    dec[...] = jnp.zeros_like(dec)
    row_pos = lax.broadcasted_iota(jnp.int32, mask.shape, 0)
    col_pos = lax.broadcasted_iota(jnp.int32, mask.shape, 1)
    mask[...] = jnp.where((col_pos <= row_pos) & (col_pos < len_ref[...]), 1.0, 0.0)

    @pl.loop(0, n_heads // 2)
    def _(g):
        att_step(2 * g, 0)
        att_step(2 * g + 1, 0)

    for g in range(RING_HEAD - 1):
        start_att(g, 1)

    pl.semaphore_wait(barrier, jnp.where(z > 0, 1, 0) + jnp.where(z < last, 1, 0))

    for d in (0, 1):
        @pl.when(pos[d] == last)
        def _():
            pltpu.make_async_copy(hb.at[d, pl.ds(0, units)], hb.at[d, pl.ds(0, units)], x_sem).wait()

    def rs_copy(d, u):
        return pltpu.make_async_remote_copy(
            src_ref=own.at[d, u % RING_OWN], dst_ref=land.at[d, u % RING_LAND],
            send_sem=rs_send.at[d, u % RING_OWN], recv_sem=rs_recv.at[d, u % RING_LAND],
            device_id={'tp': nxt[d]}, device_id_type=MESH)

    def ag_copy(d, u):
        return pltpu.make_async_remote_copy(
            src_ref=hb.at[d, u], dst_ref=hb.at[d, u],
            send_sem=ag_send.at[d, u % RING_SEND], recv_sem=ag_recv.at[d, u % RING_LAND],
            device_id={'tp': prv[d]}, device_id_type=MESH)

    def give_back(d, u):
        @pl.when(u >= RING_SEND)
        def _():
            ag_copy(d, u).wait_send()
        ag_copy(d, u).start()

    def write_out(d, u):
        w = u - units

        @pl.when((w >= 0) & (w < 4 * nt))
        def _():
            rows, cols = x_copy(d, w)
            pltpu.make_async_copy(hb.at[d, u], out_hbm.at[rows, cols], out_sem).start()

        @pl.when(w >= 4 * nt)
        def _():
            pltpu.make_async_copy(hb.at[d, u], outd_hbm.at[d, w - 4 * nt], outd_sem).start()

    def tick(t):
        for d in (0, 1):
            p = pos[d]
            u = t - LAG * p

            @pl.when((u >= 0) & (u < total))
            def _():
                @pl.when(p == 0)
                def _():
                    rs_copy(d, u).start()

                @pl.when((p > 0) & (p < last))
                def _():
                    rs_copy(d, u).wait_recv()
                    own[d, u % RING_OWN] = own[d, u % RING_OWN] + land[d, u % RING_LAND]
                    rs_copy(d, u).start()

                @pl.when(p == last)
                def _():
                    rs_copy(d, u).wait_recv()
                    summed = (own[d, u % RING_OWN] + land[d, u % RING_LAND]).astype(jnp.bfloat16)
                    hb[d, u] = (hb[d, u % units].astype(jnp.float32) + summed.astype(jnp.float32)).astype(jnp.bfloat16)
                    give_back(d, u)
                    write_out(d, u)

        for d in (0, 1):
            p = pos[d]
            v = t - LAG * (2 * last - p)

            @pl.when((p < last) & (v >= 0) & (v < total))
            def _():
                ag_copy(d, v).wait_recv()

                @pl.when(p > 0)
                def _():
                    give_back(d, v)
                write_out(d, v)

    def free_own(i):
        for d in (0, 1):
            for s in (0, 1):
                u = 2 * i + s

                @pl.when((u >= RING_OWN) & (pos[d] < last))
                def _():
                    rs_copy(d, u).wait_send()

    def store_own(i, q, res, has_dec):
        free_own(i)
        for d in (0, 1):
            for s in (0, 1):
                own[d, (2 * i + s) % RING_OWN] = res[s * SUB:(s + 1) * SUB, d * SUB:(d + 1) * SUB]
            if has_dec:
                j = q % nt
                dec[d, pl.ds(pl.multiple_of(j * DEC, DEC), DEC), :] = res[CHUNK:CHUNK + DEC, d * SUB:(d + 1) * SUB]

    def wo_step(i, q, chunk):
        start_a(q + 2)
        slot = q % 3
        pltpu.make_async_copy(wa.at[slot, pl.ds(0, hv)], wa.at[slot, pl.ds(0, hv)], wa_sem.at[slot]).wait()
        lhs = attn[0:CHUNK, :] if chunk == 0 else attn[CHUNK:2 * CHUNK + 2 * DEC, :]
        res = jnp.dot(lhs, wa[slot, 0:hv, :], preferred_element_type=jnp.float32)
        store_own(i, q, res, chunk == 1)

    def down_step(i, q, chunk):
        start_a(q + 2)
        slot = q % 3
        pltpu.make_async_copy(wa.at[slot, pl.ds(0, ffn)], wa.at[slot, pl.ds(0, ffn)], wa_sem.at[slot]).wait()
        lhs = act[chunk, 0:CHUNK, :] if chunk == 0 else act[chunk]
        res = jnp.dot(lhs, wa[slot, 0:ffn, :], preferred_element_type=jnp.float32)
        store_own(i, q, res, chunk == 1)

    def gu_step(q, chunk):
        start_b(q + 2)
        slot = q % 3
        pltpu.make_async_copy(wb.at[slot], wb.at[slot], wb_sem.at[slot]).wait()
        rows = CHUNK if chunk == 0 else CHUNK + 2 * DEC
        res = jnp.dot(b_buf[0:rows, :], wb[slot], preferred_element_type=jnp.float32)
        j = q % nf
        value = (jax.nn.silu(res[:, :SUB]) * res[:, SUB:]).astype(jnp.bfloat16)
        act[chunk, 0:rows, pl.ds(pl.multiple_of(j * SUB, SUB), SUB)] = value

    def norm_chunk(chunk):
        for s in (0, 1):
            stat[...] = jnp.zeros_like(stat)

            @pl.loop(0, nt)
            def _(j):
                for d in (0, 1):
                    hid = hb[d, 2 * (chunk * nt + j) + s].astype(jnp.float32)
                    stat[...] = stat[...] + hid * hid
            inv = lax.rsqrt(jnp.sum(stat[...], axis=-1, keepdims=True) * (1.0 / dm) + EPSILON)
            stat[...] = jnp.broadcast_to(inv, stat.shape)

            @pl.loop(0, nt)
            def _(j):
                for d in (0, 1):
                    cols = pl.ds(pl.multiple_of(d * half + j * SUB, SUB), SUB)
                    hid = hb[d, 2 * (chunk * nt + j) + s].astype(jnp.float32)
                    b_buf[s * SUB:(s + 1) * SUB, cols] = (hid * stat[...] * gain_ref[:, cols].astype(jnp.float32)).astype(jnp.bfloat16)

    def norm_dec():
        per = SUB // DEC
        tiles = []
        for d in (0, 1):
            both = [hb[d, 4 * nt + s].astype(jnp.float32) for s in (0, 1)]
            for j in range(nt):
                r = (j % per) * DEC
                tiles.append(both[j // per][r:r + DEC, :])
        square = tiles[0] * tiles[0]
        for tile in tiles[1:]:
            square = square + tile * tile
        inv = lax.rsqrt(jnp.sum(square, axis=-1, keepdims=True) * (1.0 / dm) + EPSILON)
        pad = jnp.zeros((DEC, SUB), jnp.float32)
        for k, tile in enumerate(tiles):
            value = tile * inv * gain_ref[:, k * SUB:(k + 1) * SUB].astype(jnp.float32)
            b_buf[CHUNK:CHUNK + 2 * DEC, k * SUB:(k + 1) * SUB] = jnp.concatenate([value, pad], axis=0).astype(jnp.bfloat16)

    def dec_unit(i):
        free_own(i)
        for d in (0, 1):
            for s in (0, 1):
                own[d, (2 * i + s) % RING_OWN] = dec[d, s * SUB:(s + 1) * SUB, :]

    wait_units = (2 * nt - 1 + 2 * last * LAG) // 2 + 1
    wait_all = (4 * nt + 1 + 2 * last * LAG) // 2 + 1

    @pl.loop(0, n_heads // 2)
    def _(i):
        wo_step(i, i, 0)
        tick(2 * i)
        att_step(2 * i, 1)
        tick(2 * i + 1)
        att_step(2 * i + 1, 1)

    @pl.loop(n_heads // 2, nt)
    def _(i):
        wo_step(i, i, 0)
        tick(2 * i)
        tick(2 * i + 1)

    @pl.loop(nt, wait_units)
    def _(i):
        wo_step(i, i, 1)
        tick(2 * i)
        tick(2 * i + 1)

    norm_chunk(0)
    mid0 = wait_units + nf // 2

    @pl.loop(wait_units, mid0)
    def _(i):
        wo_step(i, i, 1)
        tick(2 * i)
        gu_step(2 * (i - wait_units), 0)
        tick(2 * i + 1)
        gu_step(2 * (i - wait_units) + 1, 0)

    @pl.loop(mid0, 2 * nt)
    def _(i):
        wo_step(i, i, 1)
        tick(2 * i)
        tick(2 * i + 1)

    dec_unit(2 * nt)
    tick(4 * nt)
    tick(4 * nt + 1)

    first = 2 * nt + 1

    @pl.loop(first, wait_all)
    def _(i):
        down_step(i, i - 1, 0)
        tick(2 * i)
        tick(2 * i + 1)

    norm_chunk(1)
    norm_dec()
    mid1 = wait_all + nf // 2

    @pl.loop(wait_all, mid1)
    def _(i):
        down_step(i, i - 1, 0)
        tick(2 * i)
        gu_step(nf + 2 * (i - wait_all), 1)
        tick(2 * i + 1)
        gu_step(nf + 2 * (i - wait_all) + 1, 1)

    @pl.loop(mid1, first + nt)
    def _(i):
        down_step(i, i - 1, 0)
        tick(2 * i)
        tick(2 * i + 1)

    @pl.loop(first + nt, first + 2 * nt)
    def _(i):
        down_step(i, i - 1, 1)
        tick(2 * i)
        tick(2 * i + 1)

    dec_unit(first + 2 * nt)

    @pl.loop(total - 2, total + 2 * last * LAG)
    def _(t):
        tick(t)

    for d in (0, 1):
        @pl.when(pos[d] < last)
        def _():
            @pl.loop(total - RING_OWN, total)
            def _(u):
                rs_copy(d, u).wait_send()

        @pl.when(pos[d] > 0)
        def _():
            @pl.loop(total - RING_SEND, total)
            def _(u):
                ag_copy(d, u).wait_send()

    pltpu.make_async_copy(hb.at[:, pl.ds(units, 4 * nt)], hb.at[:, pl.ds(units, 4 * nt)], out_sem).wait()
    pltpu.make_async_copy(hb.at[:, pl.ds(0, 2)], hb.at[:, pl.ds(0, 2)], outd_sem).wait()


def finish_block(n_tp, scale, len_row, tok_len, rope_key, cos_tab, sin_tab, rot_mat, mlp_gain, normed, w_q, k_nope, value, k_tok, v_tok,
                 x_rows, y_stack, w_o, w_gate, w_up, w_down):
    seq, dm = x_rows.shape
    hv = w_o.shape[0]
    ffn = w_gate.shape[1]
    n_heads, _, nope = k_nope.shape
    vdim = value.shape[-1]
    nb, _, qk_dim, slots = k_tok.shape
    nt = dm // 2 // SUB
    units = 2 * (2 * nt + 1)
    bf, f32 = jnp.bfloat16, jnp.float32
    vmem = pl.BlockSpec(memory_space=pltpu.VMEM)
    hbm = pl.BlockSpec(memory_space=pl.ANY)
    sem = pltpu.SemaphoreType.DMA
    return pl.pallas_call(
        functools.partial(block_kernel, n_tp, n_heads, scale),
        out_shape=(jax.ShapeDtypeStruct(x_rows.shape, bf), jax.ShapeDtypeStruct((2, 2, SUB, SUB), bf)),
        in_specs=[vmem] * 8 + [hbm] * 11,
        out_specs=(hbm, hbm),
        scratch_shapes=[
            pltpu.VMEM((2, 2 * units, SUB, SUB), bf),
            pltpu.VMEM((2, RING_OWN, SUB, SUB), f32),
            pltpu.VMEM((2, RING_LAND, SUB, SUB), f32),
            pltpu.VMEM((2, CHUNK, SUB), f32),
            pltpu.VMEM((3, max(hv, ffn), 2 * SUB), bf),
            pltpu.VMEM((3, dm, 2 * SUB), bf),
            pltpu.VMEM((CHUNK + 2 * DEC, dm), bf),
            pltpu.VMEM((2, CHUNK + 2 * DEC, ffn), bf),
            pltpu.VMEM((SUB, SUB), f32),
            pltpu.VMEM((seq + 2 * DEC, hv), bf),
            pltpu.VMEM((seq, seq), f32),
            pltpu.VMEM((RING_HEAD, qk_dim, dm), bf),
            pltpu.VMEM((RING_HEAD, seq, nope), bf),
            pltpu.VMEM((RING_HEAD, seq, vdim), bf),
            pltpu.VMEM((RING_HEAD, nb, qk_dim, slots), bf),
            pltpu.VMEM((RING_HEAD, nb, slots, vdim), bf),
            sem((3,)), sem((3,)), sem, sem, sem,
            sem((2, RING_OWN)), sem((2, RING_LAND)), sem((2, RING_SEND)), sem((2, RING_LAND)), sem((3 + 2 * nb, RING_HEAD)),
        ],
        compiler_params=pltpu.CompilerParams(collective_id=0, has_side_effects=True, vmem_limit_bytes=64000 * 1024),
    )(len_row, tok_len, rope_key, cos_tab, sin_tab, rot_mat, mlp_gain, normed, w_q, k_nope, value, k_tok, v_tok, x_rows, y_stack, w_o, w_gate, w_up, w_down)


def rope_tables(positions, dim):
    half_dim = dim // 2
    inv_freq = THETA ** (-jnp.arange(half_dim, dtype=jnp.float32) * 2.0 / dim)
    angles = positions.astype(jnp.float32)[..., None] * inv_freq
    cos_part = jnp.cos(angles)
    sin_part = jnp.sin(angles)
    return jnp.concatenate([cos_part, cos_part], axis=-1), jnp.concatenate([sin_part, sin_part], axis=-1)


def rope_turn(dim):
    half_dim = dim // 2
    src = jnp.arange(dim)[:, None]
    dst = jnp.arange(dim)[None, :]
    turn = jnp.where(src == dst + half_dim, -1.0, 0.0) + jnp.where(dst == src + half_dim, 1.0, 0.0)
    return turn.astype(jnp.bfloat16)


def stack_tokens(rows):
    nb, dm = rows.shape
    nt = dm // 2 // SUB
    tiles = jnp.transpose(rows.reshape(nb, 2, nt, SUB), (1, 2, 0, 3))
    tiles = jnp.pad(tiles, ((0, 0), (0, CHUNK // DEC - nt), (0, DEC - nb), (0, 0)))
    return tiles.reshape(2, 2, SUB, SUB)


def unstack_tokens(stack, nb, dm):
    nt = dm // 2 // SUB
    tiles = stack.reshape(2, CHUNK // DEC, DEC, SUB)[:, :nt, :nb]
    return jnp.transpose(tiles, (2, 0, 1, 3)).reshape(nb, dm)


def solution(mesh):
    groups = mesh.shape['side']
    n_tp = mesh.shape['tp']
    shift_pairs = [(source_idx, (source_idx + 1) % groups) for source_idx in range(groups)]
    group_axes = ('pair', 'side')
    head_spec = P(None, None, 'tp', None)
    cache_spec = P(group_axes, None, None, None, 'tp', None)
    prompt_spec = P(group_axes, None, None, 'tp', None)
    row_spec = P(group_axes, None, None)
    spec_in = (row_spec, P(group_axes), row_spec, cache_spec, cache_spec, P(group_axes, None), P(), head_spec, P(), head_spec, head_spec, P(None, 'tp', None, None), P(), P(None, None, 'tp'), P(None, None, 'tp'), P(None, 'tp', None))
    spec_out = (row_spec, row_spec, prompt_spec, prompt_spec, cache_spec, cache_spec)

    def device_step(x_prompt, s_len, y_tok, k_cache, v_cache, c_len, attn_gain, w_q, w_dkv, w_uk, w_uv, w_o, mlp_gain, w_gate, w_up, w_down):
        hidden = x_prompt[0]
        tok_state = y_tok[0]
        seq, dm = hidden.shape
        nb = tok_state.shape[0]
        cur_len = c_len[0]
        wq, wdkv, wuk, wuv = w_q[0], w_dkv[0], w_uk[0], w_uv[0]
        nope, rank = wuk.shape[-1], wuk.shape[0]
        key_old, value_old = k_cache[0, 0], v_cache[0, 0]

        rope_dim = wq.shape[-1] - nope
        pad_rows = 2 * DEC - nb
        rows = jnp.concatenate([hidden, tok_state, jnp.zeros((pad_rows, dm), hidden.dtype)], axis=0)
        positions = jnp.concatenate([jnp.arange(seq, dtype=jnp.int32), cur_len.astype(jnp.int32), jnp.zeros((pad_rows,), jnp.int32)])
        normed = lax.optimization_barrier(rms_scaled(rows, attn_gain[0]))
        latent_pack = make_latent(normed, wdkv, positions, rank)
        received = lax.ppermute(latent_pack[:seq], 'side', shift_pairs)

        def per_head(form, left, right):
            return jnp.einsum(form, left, right, preferred_element_type=jnp.float32).astype(jnp.bfloat16)

        k_nope = per_head('sr,rhn->hsn', latent_pack[:, :rank], wuk)
        value = per_head('sr,rhv->hsv', latent_pack[:, :rank], wuv)

        tok = slice(seq, seq + nb)
        n_heads = wuk.shape[1]
        key_tok = jnp.concatenate([k_nope[:, tok], jnp.broadcast_to(latent_pack[None, tok, rank:], (n_heads, nb, rope_dim))], axis=-1)
        key_tok = jnp.transpose(key_tok, (1, 0, 2))
        value_tok = jnp.transpose(value[:, tok], (1, 0, 2))
        slot_hit = (jnp.arange(key_old.shape[1])[None, :] == cur_len[:, None])[:, :, None, None]
        key_next = jnp.where(slot_hit, key_tok[:, None], key_old)
        value_next = jnp.where(slot_hit, value_tok[:, None], value_old)

        hv = w_o.shape[1] * w_o.shape[2]
        cos_tab, sin_tab = rope_tables(positions, rope_dim)
        len_row = jnp.broadcast_to(s_len.astype(jnp.int32)[:, None], (1, seq))
        tok_len = jnp.broadcast_to(cur_len.astype(jnp.int32)[:, None], (nb, key_old.shape[1]))
        h_out, tok_out = finish_block(
            n_tp, wq.shape[-1] ** -0.5, len_row, tok_len, latent_pack[:seq, rank:], cos_tab, sin_tab, rope_turn(rope_dim), mlp_gain,
            normed, jnp.transpose(wq, (1, 2, 0)), k_nope, value, jnp.transpose(key_next, (0, 2, 3, 1)), jnp.transpose(value_next, (0, 2, 1, 3)),
            hidden, stack_tokens(tok_state), w_o[0].reshape(hv, dm), w_gate[0], w_up[0], w_down[0])

        key_in = per_head('sr,rhn->hns', received[:, :rank], wuk)
        rope_in = jnp.broadcast_to(received[:, rank:].T[None], (n_heads, rope_dim, seq))
        key_in = jnp.transpose(jnp.concatenate([key_in, rope_in], axis=1), (2, 0, 1))
        value_in = per_head('sr,rhv->shv', received[:, :rank], wuv)
        return (h_out[None], unstack_tokens(tok_out, nb, dm)[None], key_in[None, None], value_in[None, None], key_next[None, None], value_next[None, None])

    return jax.shard_map(device_step, mesh=mesh, in_specs=spec_in, out_specs=spec_out, check_vma=False)
```

```python
import functools

import jax
import jax.numpy as jnp
from jax import lax
from jax.experimental import pallas as pl
from jax.experimental.pallas import tpu as pltpu
from jax.sharding import PartitionSpec as P

EPSILON = 1e-6
THETA = 10000.0

SUB = 128
CHUNK = 2 * SUB
LAG = 2
RING_OWN = 16
RING_LAND = 32
RING_SEND = 16
RING_HEAD = 4
DEC = 8
MESH = pl.DeviceIdType.MESH


def rms_scaled(values, gain):
    hidden = values.astype(jnp.float32)
    inv_rms = lax.rsqrt(jnp.mean(hidden * hidden, axis=-1, keepdims=True) + EPSILON)
    return (hidden * inv_rms * gain.astype(jnp.float32)).astype(jnp.bfloat16)


def rms_plain(values):
    hidden = values.astype(jnp.float32)
    inv_rms = lax.rsqrt(jnp.mean(hidden * hidden, axis=-1, keepdims=True) + EPSILON)
    return (hidden * inv_rms).astype(jnp.bfloat16)


def apply_rope(values, positions):
    half_dim = values.shape[-1] // 2
    inv_freq = THETA ** (-jnp.arange(half_dim, dtype=jnp.float32) * 2.0 / values.shape[-1])
    angles = positions.astype(jnp.float32)[..., None] * inv_freq
    cos_part = jnp.cos(angles)
    sin_part = jnp.sin(angles)
    first_half = values[..., :half_dim].astype(jnp.float32)
    second_half = values[..., half_dim:].astype(jnp.float32)
    return jnp.concatenate([first_half * cos_part - second_half * sin_part, second_half * cos_part + first_half * sin_part], axis=-1).astype(jnp.bfloat16)


def make_latent(normed, w_dkv_layer, positions, rank_dim):
    latent_raw = jnp.dot(normed, w_dkv_layer, preferred_element_type=jnp.float32).astype(jnp.bfloat16)
    return jnp.concatenate([rms_plain(latent_raw[:, :rank_dim]), apply_rope(latent_raw[:, rank_dim:], positions)], axis=-1)


def block_kernel(n_tp, n_heads, scale, len_ref, clen_ref, kr_ref, cos_ref, sin_ref, rot_ref, gain_ref, a_ref,
                 wq_hbm, kn_hbm, v_hbm, kt_hbm, vt_hbm,
                 x_hbm, ys_hbm, wo_hbm, wg_hbm, wu_hbm, wd_hbm, out_hbm, outd_hbm,
                 hb, own, land, dec, wa, wb, b_buf, act, stat, attn, mask, wq_buf, kn_buf, v_buf, kt_buf, vt_buf,
                 wa_sem, wb_sem, x_sem, out_sem, outd_sem, rs_send, rs_recv, ag_send, ag_recv, att_sem):
    last = n_tp - 1
    hv = wo_hbm.shape[0]
    dm = wo_hbm.shape[1]
    ffn = wg_hbm.shape[1]
    half = dm // 2
    nt = half // SUB
    nf = ffn // SUB
    units = 2 * (2 * nt + 1)
    total = 2 * units
    z = lax.axis_index('tp')

    barrier = pltpu.get_barrier_semaphore()

    @pl.when(z > 0)
    def _():
        pl.semaphore_signal(barrier, inc=1, device_id={'tp': z - 1}, device_id_type=MESH)

    @pl.when(z < last)
    def _():
        pl.semaphore_signal(barrier, inc=1, device_id={'tp': z + 1}, device_id_type=MESH)

    pos = (z, last - z)
    nxt = (z + 1, z - 1)
    prv = (z - 1, z + 1)

    def wo_copies(q):
        slot = q % 3
        j = q % nt
        return [pltpu.make_async_copy(wo_hbm.at[:, pl.ds(pl.multiple_of(d * half + j * SUB, SUB), SUB)],
                                      wa.at[slot, pl.ds(0, hv), pl.ds(d * SUB, SUB)], wa_sem.at[slot]) for d in (0, 1)]

    def wd_copies(q):
        slot = q % 3
        j = q % nt
        return [pltpu.make_async_copy(wd_hbm.at[:, pl.ds(pl.multiple_of(d * half + j * SUB, SUB), SUB)],
                                      wa.at[slot, pl.ds(0, ffn), pl.ds(d * SUB, SUB)], wa_sem.at[slot]) for d in (0, 1)]

    def start_a(q):
        @pl.when(q < 2 * nt)
        def _():
            for copy in wo_copies(q):
                copy.start()

        @pl.when((q >= 2 * nt) & (q < 4 * nt))
        def _():
            for copy in wd_copies(q):
                copy.start()

    def start_b(q):
        @pl.when(q < 2 * nf)
        def _():
            slot = q % 3
            j = q % nf
            cols = pl.ds(pl.multiple_of(j * SUB, SUB), SUB)
            pltpu.make_async_copy(wg_hbm.at[:, cols], wb.at[slot, :, pl.ds(0, SUB)], wb_sem.at[slot]).start()
            pltpu.make_async_copy(wu_hbm.at[:, cols], wb.at[slot, :, pl.ds(SUB, SUB)], wb_sem.at[slot]).start()

    nope = kn_hbm.shape[-1]
    nb = kt_hbm.shape[0]
    tok_rows = slice(2 * CHUNK, 2 * CHUNK + 2 * DEC)

    def att_copies(g, chunk):
        slot = g % RING_HEAD
        keys = pl.ds(0, CHUNK * (chunk + 1))
        copies = [pltpu.make_async_copy(wq_hbm.at[g], wq_buf.at[slot], att_sem.at[0, slot]),
                  pltpu.make_async_copy(kn_hbm.at[g, keys], kn_buf.at[slot, keys], att_sem.at[1, slot]),
                  pltpu.make_async_copy(v_hbm.at[g, keys], v_buf.at[slot, keys], att_sem.at[2, slot])]
        if chunk == 0:
            for n in range(nb):
                copies.append(pltpu.make_async_copy(kt_hbm.at[n, g], kt_buf.at[slot, n], att_sem.at[3 + n, slot]))
                copies.append(pltpu.make_async_copy(vt_hbm.at[n, g], vt_buf.at[slot, n], att_sem.at[3 + nb + n, slot]))
        return copies

    def start_att(g, chunk):
        for copy in att_copies(g, chunk):
            copy.start()

    def take_rows(ref, chunk):
        if chunk == 0:
            return jnp.concatenate([ref[0:CHUNK, :], ref[tok_rows, :]], axis=0)
        return ref[CHUNK:2 * CHUNK, :]

    def softmax(scores):
        expd = jnp.exp(scores - jnp.max(scores, axis=-1, keepdims=True))
        return (expd * (1.0 / jnp.sum(expd, axis=-1, keepdims=True))).astype(jnp.bfloat16)

    def att_pair(g, chunk):
        @pl.when(g + 2 < n_heads)
        def _():
            start_att(g + 2, chunk)
            start_att(g + 3, chunk)
        for k in (0, 1):
            for copy in att_copies(g + k, chunk):
                copy.wait()
        queries = [project(g + k, chunk) for k in (0, 1)]
        for k in (0, 1):
            attend(g + k, chunk, *queries[k])

    def project(g, chunk):
        contract = (((1,), (1,)), ((), ()))
        f32, bf = jnp.float32, jnp.bfloat16
        query = lax.dot_general(take_rows(a_ref, chunk), wq_buf[g % RING_HEAD], contract, preferred_element_type=f32).astype(bf)
        flat, raw = query[:, :nope], query[:, nope:]
        turned = jnp.dot(raw, rot_ref[...], preferred_element_type=f32)
        rope = (raw.astype(f32) * take_rows(cos_ref, chunk) + turned * take_rows(sin_ref, chunk)).astype(bf)
        return flat, rope

    def attend(g, chunk, flat, rope):
        slot = g % RING_HEAD
        keys = CHUNK * (chunk + 1)
        rows = slice(chunk * CHUNK, (chunk + 1) * CHUNK)
        cols = pl.ds(pl.multiple_of(g * SUB, SUB), SUB)
        contract = (((1,), (1,)), ((), ()))
        f32, bf = jnp.float32, jnp.bfloat16
        scores = lax.dot_general(flat[:CHUNK], kn_buf[slot, 0:keys, :], contract, preferred_element_type=f32)
        scores = scores + lax.dot_general(rope[:CHUNK], kr_ref[0:keys, :], contract, preferred_element_type=f32)
        probs = softmax(jnp.where(mask[rows, 0:keys] > 0, scores * scale, -1e30))
        attn[rows, cols] = jnp.dot(probs, v_buf[slot, 0:keys, :], preferred_element_type=f32).astype(bf)
        if chunk == 0:
            total_tok = jnp.zeros((2 * DEC, SUB), f32)
            for n in range(nb):
                kt = kt_buf[slot, n]
                scores = jnp.dot(flat[CHUNK:], kt[:nope], preferred_element_type=f32)
                scores = (scores + jnp.dot(rope[CHUNK:], kt[nope:], preferred_element_type=f32)) * scale
                slots = lax.broadcasted_iota(jnp.int32, scores.shape, 1)
                probs = softmax(jnp.where(slots <= clen_ref[n:n + 1, :], scores, -1e30))
                value = jnp.dot(probs, vt_buf[slot, n], preferred_element_type=f32)
                row = lax.broadcasted_iota(jnp.int32, value.shape, 0)
                total_tok = jnp.where(row == n, value, total_tok)
            attn[tok_rows, cols] = total_tok.astype(bf)

    for g in (0, 1):
        start_att(g, 0)
    start_a(0)
    start_a(1)
    start_b(0)
    start_b(1)

    def x_copy(d, w):
        i = w // 2
        rows = pl.ds(pl.multiple_of((i // nt) * CHUNK + (w % 2) * SUB, SUB), SUB)
        cols = pl.ds(pl.multiple_of(d * half + (i % nt) * SUB, SUB), SUB)
        return rows, cols

    for d in (0, 1):
        @pl.when(pos[d] == last)
        def _():
            @pl.loop(0, 4 * nt)
            def _(w):
                rows, cols = x_copy(d, w)
                pltpu.make_async_copy(x_hbm.at[rows, cols], hb.at[d, w], x_sem).start()
            for s in (0, 1):
                pltpu.make_async_copy(ys_hbm.at[d, s], hb.at[d, 4 * nt + s], x_sem).start()

    dec[...] = jnp.zeros_like(dec)
    row_pos = lax.broadcasted_iota(jnp.int32, mask.shape, 0)
    col_pos = lax.broadcasted_iota(jnp.int32, mask.shape, 1)
    mask[...] = jnp.where((col_pos <= row_pos) & (col_pos < len_ref[...]), 1.0, 0.0)

    @pl.loop(0, n_heads // 2)
    def _(g):
        att_pair(2 * g, 0)

    for g in (0, 1):
        start_att(g, 1)

    pl.semaphore_wait(barrier, jnp.where(z > 0, 1, 0) + jnp.where(z < last, 1, 0))

    for d in (0, 1):
        @pl.when(pos[d] == last)
        def _():
            pltpu.make_async_copy(hb.at[d, pl.ds(0, units)], hb.at[d, pl.ds(0, units)], x_sem).wait()

    def rs_copy(d, u):
        return pltpu.make_async_remote_copy(
            src_ref=own.at[d, u % RING_OWN], dst_ref=land.at[d, u % RING_LAND],
            send_sem=rs_send.at[d, u % RING_OWN], recv_sem=rs_recv.at[d, u % RING_LAND],
            device_id={'tp': nxt[d]}, device_id_type=MESH)

    def ag_copy(d, u):
        return pltpu.make_async_remote_copy(
            src_ref=hb.at[d, u], dst_ref=hb.at[d, u],
            send_sem=ag_send.at[d, u % RING_SEND], recv_sem=ag_recv.at[d, u % RING_LAND],
            device_id={'tp': prv[d]}, device_id_type=MESH)

    def give_back(d, u):
        @pl.when(u >= RING_SEND)
        def _():
            ag_copy(d, u).wait_send()
        ag_copy(d, u).start()

    def write_out(d, u):
        w = u - units

        @pl.when((w >= 0) & (w < 4 * nt))
        def _():
            rows, cols = x_copy(d, w)
            pltpu.make_async_copy(hb.at[d, u], out_hbm.at[rows, cols], out_sem).start()

        @pl.when(w >= 4 * nt)
        def _():
            pltpu.make_async_copy(hb.at[d, u], outd_hbm.at[d, w - 4 * nt], outd_sem).start()

    def tick(t):
        for d in (0, 1):
            p = pos[d]
            u = t - LAG * p

            @pl.when((u >= 0) & (u < total))
            def _():
                @pl.when(p == 0)
                def _():
                    rs_copy(d, u).start()

                @pl.when((p > 0) & (p < last))
                def _():
                    rs_copy(d, u).wait_recv()
                    own[d, u % RING_OWN] = own[d, u % RING_OWN] + land[d, u % RING_LAND]
                    rs_copy(d, u).start()

                @pl.when(p == last)
                def _():
                    rs_copy(d, u).wait_recv()
                    summed = (own[d, u % RING_OWN] + land[d, u % RING_LAND]).astype(jnp.bfloat16)
                    hb[d, u] = (hb[d, u % units].astype(jnp.float32) + summed.astype(jnp.float32)).astype(jnp.bfloat16)
                    give_back(d, u)
                    write_out(d, u)

        for d in (0, 1):
            p = pos[d]
            v = t - LAG * (2 * last - p)

            @pl.when((p < last) & (v >= 0) & (v < total))
            def _():
                ag_copy(d, v).wait_recv()

                @pl.when(p > 0)
                def _():
                    give_back(d, v)
                write_out(d, v)

    def free_own(i):
        for d in (0, 1):
            for s in (0, 1):
                u = 2 * i + s

                @pl.when((u >= RING_OWN) & (pos[d] < last))
                def _():
                    rs_copy(d, u).wait_send()

    def store_own(i, q, res, has_dec):
        free_own(i)
        for d in (0, 1):
            for s in (0, 1):
                own[d, (2 * i + s) % RING_OWN] = res[s * SUB:(s + 1) * SUB, d * SUB:(d + 1) * SUB]
            if has_dec:
                j = q % nt
                dec[d, pl.ds(pl.multiple_of(j * DEC, DEC), DEC), :] = res[CHUNK:CHUNK + DEC, d * SUB:(d + 1) * SUB]

    def wo_step(i, q, chunk):
        start_a(q + 2)
        slot = q % 3
        pltpu.make_async_copy(wa.at[slot, pl.ds(0, hv)], wa.at[slot, pl.ds(0, hv)], wa_sem.at[slot]).wait()
        lhs = attn[0:CHUNK, :] if chunk == 0 else attn[CHUNK:2 * CHUNK + 2 * DEC, :]
        res = jnp.dot(lhs, wa[slot, 0:hv, :], preferred_element_type=jnp.float32)
        store_own(i, q, res, chunk == 1)

    def down_step(i, q, chunk):
        start_a(q + 2)
        slot = q % 3
        pltpu.make_async_copy(wa.at[slot, pl.ds(0, ffn)], wa.at[slot, pl.ds(0, ffn)], wa_sem.at[slot]).wait()
        lhs = act[chunk, 0:CHUNK, :] if chunk == 0 else act[chunk]
        res = jnp.dot(lhs, wa[slot, 0:ffn, :], preferred_element_type=jnp.float32)
        store_own(i, q, res, chunk == 1)

    def gu_step(q, chunk):
        start_b(q + 2)
        slot = q % 3
        pltpu.make_async_copy(wb.at[slot], wb.at[slot], wb_sem.at[slot]).wait()
        rows = CHUNK if chunk == 0 else CHUNK + 2 * DEC
        res = jnp.dot(b_buf[0:rows, :], wb[slot], preferred_element_type=jnp.float32)
        j = q % nf
        value = (jax.nn.silu(res[:, :SUB]) * res[:, SUB:]).astype(jnp.bfloat16)
        act[chunk, 0:rows, pl.ds(pl.multiple_of(j * SUB, SUB), SUB)] = value

    def norm_chunk(chunk):
        for s in (0, 1):
            stat[...] = jnp.zeros_like(stat)

            @pl.loop(0, nt)
            def _(j):
                for d in (0, 1):
                    hid = hb[d, 2 * (chunk * nt + j) + s].astype(jnp.float32)
                    stat[...] = stat[...] + hid * hid
            inv = lax.rsqrt(jnp.sum(stat[...], axis=-1, keepdims=True) * (1.0 / dm) + EPSILON)
            stat[...] = jnp.broadcast_to(inv, stat.shape)

            @pl.loop(0, nt)
            def _(j):
                for d in (0, 1):
                    cols = pl.ds(pl.multiple_of(d * half + j * SUB, SUB), SUB)
                    hid = hb[d, 2 * (chunk * nt + j) + s].astype(jnp.float32)
                    b_buf[s * SUB:(s + 1) * SUB, cols] = (hid * stat[...] * gain_ref[:, cols].astype(jnp.float32)).astype(jnp.bfloat16)

    def norm_dec():
        per = SUB // DEC
        tiles = []
        for d in (0, 1):
            both = [hb[d, 4 * nt + s].astype(jnp.float32) for s in (0, 1)]
            for j in range(nt):
                r = (j % per) * DEC
                tiles.append(both[j // per][r:r + DEC, :])
        square = tiles[0] * tiles[0]
        for tile in tiles[1:]:
            square = square + tile * tile
        inv = lax.rsqrt(jnp.sum(square, axis=-1, keepdims=True) * (1.0 / dm) + EPSILON)
        pad = jnp.zeros((DEC, SUB), jnp.float32)
        for k, tile in enumerate(tiles):
            value = tile * inv * gain_ref[:, k * SUB:(k + 1) * SUB].astype(jnp.float32)
            b_buf[CHUNK:CHUNK + 2 * DEC, k * SUB:(k + 1) * SUB] = jnp.concatenate([value, pad], axis=0).astype(jnp.bfloat16)

    def dec_unit(i):
        free_own(i)
        for d in (0, 1):
            for s in (0, 1):
                own[d, (2 * i + s) % RING_OWN] = dec[d, s * SUB:(s + 1) * SUB, :]

    wait_units = (2 * nt - 1 + 2 * last * LAG) // 2 + 1
    wait_all = (4 * nt + 1 + 2 * last * LAG) // 2 + 1

    @pl.loop(0, n_heads // 2)
    def _(i):
        wo_step(i, i, 0)
        tick(2 * i)
        att_pair(2 * i, 1)
        tick(2 * i + 1)

    @pl.loop(n_heads // 2, nt)
    def _(i):
        wo_step(i, i, 0)
        tick(2 * i)
        tick(2 * i + 1)

    @pl.loop(nt, wait_units)
    def _(i):
        wo_step(i, i, 1)
        tick(2 * i)
        tick(2 * i + 1)

    norm_chunk(0)
    mid0 = wait_units + nf // 2

    @pl.loop(wait_units, mid0)
    def _(i):
        wo_step(i, i, 1)
        tick(2 * i)
        gu_step(2 * (i - wait_units), 0)
        tick(2 * i + 1)
        gu_step(2 * (i - wait_units) + 1, 0)

    @pl.loop(mid0, 2 * nt)
    def _(i):
        wo_step(i, i, 1)
        tick(2 * i)
        tick(2 * i + 1)

    dec_unit(2 * nt)
    tick(4 * nt)
    tick(4 * nt + 1)

    first = 2 * nt + 1

    @pl.loop(first, wait_all)
    def _(i):
        down_step(i, i - 1, 0)
        tick(2 * i)
        tick(2 * i + 1)

    norm_chunk(1)
    norm_dec()
    mid1 = wait_all + nf // 2

    @pl.loop(wait_all, mid1)
    def _(i):
        down_step(i, i - 1, 0)
        tick(2 * i)
        gu_step(nf + 2 * (i - wait_all), 1)
        tick(2 * i + 1)
        gu_step(nf + 2 * (i - wait_all) + 1, 1)

    @pl.loop(mid1, first + nt)
    def _(i):
        down_step(i, i - 1, 0)
        tick(2 * i)
        tick(2 * i + 1)

    @pl.loop(first + nt, first + 2 * nt)
    def _(i):
        down_step(i, i - 1, 1)
        tick(2 * i)
        tick(2 * i + 1)

    dec_unit(first + 2 * nt)

    @pl.loop(total - 2, total + 2 * last * LAG)
    def _(t):
        tick(t)

    for d in (0, 1):
        @pl.when(pos[d] < last)
        def _():
            @pl.loop(total - RING_OWN, total)
            def _(u):
                rs_copy(d, u).wait_send()

        @pl.when(pos[d] > 0)
        def _():
            @pl.loop(total - RING_SEND, total)
            def _(u):
                ag_copy(d, u).wait_send()

    pltpu.make_async_copy(hb.at[:, pl.ds(units, 4 * nt)], hb.at[:, pl.ds(units, 4 * nt)], out_sem).wait()
    pltpu.make_async_copy(hb.at[:, pl.ds(0, 2)], hb.at[:, pl.ds(0, 2)], outd_sem).wait()


def finish_block(n_tp, scale, len_row, tok_len, rope_key, cos_tab, sin_tab, rot_mat, mlp_gain, normed, w_q, k_nope, value, k_tok, v_tok,
                 x_rows, y_stack, w_o, w_gate, w_up, w_down):
    seq, dm = x_rows.shape
    hv = w_o.shape[0]
    ffn = w_gate.shape[1]
    n_heads, _, nope = k_nope.shape
    vdim = value.shape[-1]
    nb, _, qk_dim, slots = k_tok.shape
    nt = dm // 2 // SUB
    units = 2 * (2 * nt + 1)
    bf, f32 = jnp.bfloat16, jnp.float32
    vmem = pl.BlockSpec(memory_space=pltpu.VMEM)
    hbm = pl.BlockSpec(memory_space=pl.ANY)
    sem = pltpu.SemaphoreType.DMA
    return pl.pallas_call(
        functools.partial(block_kernel, n_tp, n_heads, scale),
        out_shape=(jax.ShapeDtypeStruct(x_rows.shape, bf), jax.ShapeDtypeStruct((2, 2, SUB, SUB), bf)),
        in_specs=[vmem] * 8 + [hbm] * 11,
        out_specs=(hbm, hbm),
        scratch_shapes=[
            pltpu.VMEM((2, 2 * units, SUB, SUB), bf),
            pltpu.VMEM((2, RING_OWN, SUB, SUB), f32),
            pltpu.VMEM((2, RING_LAND, SUB, SUB), f32),
            pltpu.VMEM((2, CHUNK, SUB), f32),
            pltpu.VMEM((3, max(hv, ffn), 2 * SUB), bf),
            pltpu.VMEM((3, dm, 2 * SUB), bf),
            pltpu.VMEM((CHUNK + 2 * DEC, dm), bf),
            pltpu.VMEM((2, CHUNK + 2 * DEC, ffn), bf),
            pltpu.VMEM((SUB, SUB), f32),
            pltpu.VMEM((seq + 2 * DEC, hv), bf),
            pltpu.VMEM((seq, seq), f32),
            pltpu.VMEM((RING_HEAD, qk_dim, dm), bf),
            pltpu.VMEM((RING_HEAD, seq, nope), bf),
            pltpu.VMEM((RING_HEAD, seq, vdim), bf),
            pltpu.VMEM((RING_HEAD, nb, qk_dim, slots), bf),
            pltpu.VMEM((RING_HEAD, nb, slots, vdim), bf),
            sem((3,)), sem((3,)), sem, sem, sem,
            sem((2, RING_OWN)), sem((2, RING_LAND)), sem((2, RING_SEND)), sem((2, RING_LAND)), sem((3 + 2 * nb, RING_HEAD)),
        ],
        compiler_params=pltpu.CompilerParams(collective_id=0, has_side_effects=True, vmem_limit_bytes=64000 * 1024),
    )(len_row, tok_len, rope_key, cos_tab, sin_tab, rot_mat, mlp_gain, normed, w_q, k_nope, value, k_tok, v_tok, x_rows, y_stack, w_o, w_gate, w_up, w_down)


def rope_tables(positions, dim):
    half_dim = dim // 2
    inv_freq = THETA ** (-jnp.arange(half_dim, dtype=jnp.float32) * 2.0 / dim)
    angles = positions.astype(jnp.float32)[..., None] * inv_freq
    cos_part = jnp.cos(angles)
    sin_part = jnp.sin(angles)
    return jnp.concatenate([cos_part, cos_part], axis=-1), jnp.concatenate([sin_part, sin_part], axis=-1)


def rope_turn(dim):
    half_dim = dim // 2
    src = jnp.arange(dim)[:, None]
    dst = jnp.arange(dim)[None, :]
    turn = jnp.where(src == dst + half_dim, -1.0, 0.0) + jnp.where(dst == src + half_dim, 1.0, 0.0)
    return turn.astype(jnp.bfloat16)


def stack_tokens(rows):
    nb, dm = rows.shape
    nt = dm // 2 // SUB
    tiles = jnp.transpose(rows.reshape(nb, 2, nt, SUB), (1, 2, 0, 3))
    tiles = jnp.pad(tiles, ((0, 0), (0, CHUNK // DEC - nt), (0, DEC - nb), (0, 0)))
    return tiles.reshape(2, 2, SUB, SUB)


def unstack_tokens(stack, nb, dm):
    nt = dm // 2 // SUB
    tiles = stack.reshape(2, CHUNK // DEC, DEC, SUB)[:, :nt, :nb]
    return jnp.transpose(tiles, (2, 0, 1, 3)).reshape(nb, dm)


def solution(mesh):
    groups = mesh.shape['side']
    n_tp = mesh.shape['tp']
    shift_pairs = [(source_idx, (source_idx + 1) % groups) for source_idx in range(groups)]
    group_axes = ('pair', 'side')
    head_spec = P(None, None, 'tp', None)
    cache_spec = P(group_axes, None, None, None, 'tp', None)
    prompt_spec = P(group_axes, None, None, 'tp', None)
    row_spec = P(group_axes, None, None)
    spec_in = (row_spec, P(group_axes), row_spec, cache_spec, cache_spec, P(group_axes, None), P(), head_spec, P(), head_spec, head_spec, P(None, 'tp', None, None), P(), P(None, None, 'tp'), P(None, None, 'tp'), P(None, 'tp', None))
    spec_out = (row_spec, row_spec, prompt_spec, prompt_spec, cache_spec, cache_spec)

    def device_step(x_prompt, s_len, y_tok, k_cache, v_cache, c_len, attn_gain, w_q, w_dkv, w_uk, w_uv, w_o, mlp_gain, w_gate, w_up, w_down):
        hidden = x_prompt[0]
        tok_state = y_tok[0]
        seq, dm = hidden.shape
        nb = tok_state.shape[0]
        cur_len = c_len[0]
        wq, wdkv, wuk, wuv = w_q[0], w_dkv[0], w_uk[0], w_uv[0]
        nope, rank = wuk.shape[-1], wuk.shape[0]
        key_old, value_old = k_cache[0, 0], v_cache[0, 0]

        rope_dim = wq.shape[-1] - nope
        pad_rows = 2 * DEC - nb
        rows = jnp.concatenate([hidden, tok_state, jnp.zeros((pad_rows, dm), hidden.dtype)], axis=0)
        positions = jnp.concatenate([jnp.arange(seq, dtype=jnp.int32), cur_len.astype(jnp.int32), jnp.zeros((pad_rows,), jnp.int32)])
        normed = lax.optimization_barrier(rms_scaled(rows, attn_gain[0]))
        latent_pack = make_latent(normed, wdkv, positions, rank)
        received = lax.ppermute(latent_pack[:seq], 'side', shift_pairs)

        def per_head(form, left, right):
            return jnp.einsum(form, left, right, preferred_element_type=jnp.float32).astype(jnp.bfloat16)

        k_nope = per_head('sr,rhn->hsn', latent_pack[:, :rank], wuk)
        value = per_head('sr,rhv->hsv', latent_pack[:, :rank], wuv)

        tok = slice(seq, seq + nb)
        n_heads = wuk.shape[1]
        key_tok = jnp.concatenate([k_nope[:, tok], jnp.broadcast_to(latent_pack[None, tok, rank:], (n_heads, nb, rope_dim))], axis=-1)
        key_tok = jnp.transpose(key_tok, (1, 0, 2))
        value_tok = jnp.transpose(value[:, tok], (1, 0, 2))
        slot_hit = (jnp.arange(key_old.shape[1])[None, :] == cur_len[:, None])[:, :, None, None]
        key_next = lax.optimization_barrier(jnp.transpose(jnp.where(slot_hit, key_tok[:, None], key_old), (0, 2, 3, 1)))
        value_next = jnp.where(slot_hit, value_tok[:, None], value_old)

        hv = w_o.shape[1] * w_o.shape[2]
        cos_tab, sin_tab = rope_tables(positions, rope_dim)
        len_row = jnp.broadcast_to(s_len.astype(jnp.int32)[:, None], (1, seq))
        tok_len = jnp.broadcast_to(cur_len.astype(jnp.int32)[:, None], (nb, key_old.shape[1]))
        h_out, tok_out = finish_block(
            n_tp, wq.shape[-1] ** -0.5, len_row, tok_len, latent_pack[:seq, rank:], cos_tab, sin_tab, rope_turn(rope_dim), mlp_gain,
            normed, jnp.transpose(wq, (1, 2, 0)), k_nope, value, key_next, jnp.transpose(value_next, (0, 2, 1, 3)),
            hidden, stack_tokens(tok_state), w_o[0].reshape(hv, dm), w_gate[0], w_up[0], w_down[0])

        key_in = per_head('sr,rhn->hns', received[:, :rank], wuk)
        rope_in = jnp.broadcast_to(received[:, rank:].T[None], (n_heads, rope_dim, seq))
        key_in = jnp.transpose(jnp.concatenate([key_in, rope_in], axis=1), (2, 0, 1))
        value_in = per_head('sr,rhv->shv', received[:, :rank], wuv)
        return (h_out[None], unstack_tokens(tok_out, nb, dm)[None], key_in[None, None], value_in[None, None], jnp.transpose(key_next, (0, 3, 1, 2))[None, None], value_next[None, None])

    return jax.shard_map(device_step, mesh=mesh, in_specs=spec_in, out_specs=spec_out, check_vma=False)
```
